256 devices in a mesh: seq: 64 (over z, y, core), head: 4 (over x).
Axes of the slice: x: 4, y: 4, z: 8, core: 2. Of those that a mesh axis runs over, the one named last changes fastest.
Arguments:
- tail_queries: bfloat16 [10, 64, 4096], P(None, 'seq', 'head'), may hold values from -8 to 8
- keys: bfloat16 [10, 131072, 1024], P(None, 'seq', 'head'), may hold values from -160 to 160
Outputs:
- vertical: float32 [10, 32, 131072], P(None, 'head', 'seq')
- slash: float32 [10, 32, 131072], P(None, 'head', 'seq')
The draws below stay inside these ranges and needn't reach their ends.
All inputs are finite; a program needn't handle non-finite values.
Results may differ from the reference program's by a relative error of at most 0.0003.
Values may be sent and summed in bfloat16 or wider, within the bound.
A program may use at most 64 MiB of HBM per device.

```python
import math
import jax
import jax.numpy as jnp
from jax import lax

HD = 128
HEADS = 32
KV_HEADS = 8
LAST = 64
LAYERS = 10
TOKENS = 131072


def query_field(key):
    return jax.random.normal(jax.random.fold_in(key, 11), (LAYERS, LAST, HEADS * HD), jnp.float32)


def draw_tail_queries(key, part):
    return query_field(key).astype(jnp.bfloat16)


def draw_keys(key, part):
    normal_keys = jax.random.normal(jax.random.fold_in(key, 23), (LAYERS, TOKENS, KV_HEADS * HD), jnp.float32)
    return normal_keys.astype(jnp.bfloat16)


def setup_inputs(seed: int = 0) -> dict:
    streams_of = jax.random.split(jax.random.key(seed), 3)
    return {
        "tail_queries": draw_tail_queries(jax.random.fold_in(streams_of[2], 71), 0),
        "keys": draw_keys(jax.random.fold_in(streams_of[2], 71), 0),
    }


def diagonal_sums(probabilities):
    head_count, query_count, key_count = probabilities.shape
    width = key_count + (query_count + 127) // 128 * 128
    rows = jnp.pad(probabilities[:, ::-1, :], ((0, 0), (0, 0), (0, width - key_count)))
    offset = 1
    while rows.shape[1] > 1:
        if rows.shape[1] % 2 == 1:
            rows = jnp.pad(rows, ((0, 0), (0, 1), (0, 0)))
        even_rows = rows[:, 0::2, :]
        odd_rows = rows[:, 1::2, :]
        odd_rows = jnp.pad(odd_rows[:, :, :width - offset], ((0, 0), (0, 0), (offset, 0)))
        rows = even_rows + odd_rows
        offset = offset * 2
    return rows[:, 0, :key_count + query_count]

def group_sums(inputs):
    queries, group_keys = inputs
    scores = jnp.einsum('qad,kd->aqk', queries.astype(jnp.float32), group_keys.astype(jnp.float32), precision=lax.Precision.HIGHEST)
    scores = scores * (1.0 / math.sqrt(HD))
    positions = TOKENS - LAST + jnp.arange(LAST)
    visible = jnp.arange(TOKENS)[None, :] <= positions[:, None]
    scores = jnp.where(visible[None], scores, -jnp.inf)
    row_max = lax.optimization_barrier(jnp.max(scores, axis=2, keepdims=True))
    weights = jnp.exp(scores - row_max)
    row_total = lax.optimization_barrier(jnp.sum(weights, axis=2, keepdims=True))
    probabilities = weights / row_total
    ratio = TOKENS / LAST
    vertical = lax.optimization_barrier(jnp.sum(probabilities, axis=1)) * ratio
    slash = diagonal_sums(probabilities)[:, :TOKENS] * ratio
    return (vertical, slash)

def layer_sums(inputs):
    queries, layer_keys = inputs
    per_group = HEADS // KV_HEADS
    grouped_queries = queries.reshape(LAST, KV_HEADS, per_group, HD).transpose(1, 0, 2, 3)
    grouped_keys = layer_keys.reshape(TOKENS, KV_HEADS, HD).transpose(1, 0, 2)
    vertical, slash = lax.map(group_sums, (grouped_queries, grouped_keys))
    return (vertical.reshape(HEADS, TOKENS), slash.reshape(HEADS, TOKENS))

def reference(tail_queries, keys):
    vertical, slash = lax.map(layer_sums, (tail_queries, keys))
    return (vertical, slash)
```

```python
import functools
import math

import jax
import jax.numpy as jnp
from jax import lax
from jax.experimental import pallas as pl
from jax.experimental.pallas import tpu as pltpu
from jax.sharding import PartitionSpec as P

HD = 128
LAST = 64
LANES = 128
F32 = jnp.float32
BF16 = jnp.bfloat16
SCALE = math.log2(math.e) / math.sqrt(HD)
CHUNK = 2
NZ, NY, NC = 8, 4, 2
NR = NY * NC


def tree(op, xs):
    xs = list(xs)
    while len(xs) > 1:
        xs = [op(*xs[n : n + 2]) if n + 1 < len(xs) else xs[n] for n in range(0, len(xs), 2)]
    return xs[0]


def combined(parts):
    top = tree(jnp.maximum, parts)
    return top + jnp.log2(tree(jnp.add, [jnp.exp2(part - top) for part in parts]))


def score(q, k_ref, layer, group, s_ref):
    keys = s_ref.shape[1]
    for n in range(0, keys, 256):
        k = k_ref[layer, n : n + 256, HD * group : HD * group + HD]
        s_ref[:, n : n + 256] = lax.dot_general(
            q, k, (((1,), (1,)), ((), ())), preferred_element_type=F32
        )


def weigh(s_ref, w_ref, m_ref, t_ref, limit):
    rows, keys = s_ref.shape
    lane = lax.broadcasted_iota(jnp.int32, (8, LANES), 1)
    sub = lax.broadcasted_iota(jnp.int32, (8, LANES), 0)
    ahead = lane - jnp.where(sub >= 4, 1, 0)
    for v in range(rows // 8):
        at = slice(8 * v, 8 * v + 8)
        xs = [s_ref[at, n : n + LANES] for n in range(0, keys, LANES)]
        xs[-1] = jnp.where(ahead > limit + 2 * v, -jnp.inf, xs[-1])
        top = tree(jnp.maximum, xs)
        ws = [jnp.exp2((x - top) * SCALE) for x in xs]
        for n, w in enumerate(ws):
            w_ref[at, n * LANES : n * LANES + LANES] = w
        m_ref[at, :] = top
        t_ref[at, :] = tree(jnp.add, ws)


def row_stats(m_ref, t_ref, mt_ref):
    mt = m_ref[...].T
    mt_ref[...] = mt
    top = jnp.max(mt, axis=0, keepdims=True)
    total = jnp.sum(t_ref[...].T * jnp.exp2((mt - top) * SCALE), axis=0, keepdims=True)
    return top * SCALE + jnp.log2(total)


def spread(w_ref, f_ref, vert_ref, slash_ref, over_ref, group):
    rows, keys = w_ref.shape
    tiles = keys // LANES
    lane = lax.broadcasted_iota(jnp.int32, (8, LANES), 1)
    zero = jnp.zeros((8, LANES), F32)
    vert = [zero] * tiles
    slash = [zero] * (tiles + 1)
    for v in range(rows // 8):
        at = slice(8 * v, 8 * v + 8)
        shift = LAST - 2 - 2 * v
        factor = f_ref[at, :]
        wrapped = lane < shift
        before = zero
        for n in range(tiles):
            p = w_ref[at, n * LANES : n * LANES + LANES] * factor
            vert[n] = vert[n] + p
            if shift:
                turned = pltpu.roll(p, shift, 1)
                p = jnp.where(wrapped, before, turned)
                before = turned
            slash[n] = slash[n] + p
        if shift:
            slash[tiles] = slash[tiles] + jnp.where(wrapped, before, 0.0)
    before = zero
    heads = slice(4 * group, 4 * group + 4)
    for n in range(tiles + 1):
        turned = pltpu.roll(slash[n], 1, 1)
        y = jnp.where(lane < 1, before, turned)[0:4] + slash[n][4:8]
        before = turned
        if n < tiles:
            slash_ref[heads, n * LANES : n * LANES + LANES] = y
            vert_ref[heads, n * LANES : n * LANES + LANES] = vert[n][0:4] + vert[n][4:8]
        else:
            over_ref[heads, :] = y


def kernel(
    q_hbm, k_hbm, vert_hbm, slash_hbm,
    qg, kv, sa, sb, wv, mv, tv, mt, fv, vo, so, over, over_in, st1, st2, total,
    q_sem, k_sem, o_sem,
    z_send, z_recv, y_send, y_recv, c_send, c_recv,
    s1_send, s1_recv, s2_send, s2_recv, d_send, d_recv,
):
    layers = kv.shape[0]
    chunks = layers // CHUNK
    seq = lax.axis_index("seq")
    z, r = seq // NR, lax.rem(seq, NR)
    y, c = r // NC, lax.rem(r, NC)
    z_peer = lambda n: lax.rem(z + n, NZ) * NR + r
    r_peer = lambda n: z * NR + lax.rem(r + n, NR)
    ahead, behind = lax.rem(seq + 1, NZ * NR), lax.rem(seq + NZ * NR - 1, NZ * NR)
    count = lax.axis_size("seq")
    limit = LAST + jnp.where(seq == count - 1, 0, 1000)

    own = pltpu.make_async_copy(q_hbm, qg.at[z, y, c], q_sem)
    own.start()
    key_copy = lambda n: pltpu.make_async_copy(k_hbm.at[n], kv.at[n], k_sem.at[n])
    for n in range(layers):
        key_copy(n).start()

    barrier = pltpu.get_barrier_semaphore()
    greeted = [z_peer(n) for n in range(1, NZ)] + [r_peer(n) for n in range(1, NR)] + [ahead, behind]
    for peer in greeted:
        pl.semaphore_signal(barrier, inc=1, device_id={"seq": peer}, device_id_type=pl.DeviceIdType.MESH)

    def remote(src, dst, send, recv, peer):
        return pltpu.make_async_remote_copy(
            src_ref=src, dst_ref=dst, send_sem=send, recv_sem=recv,
            device_id={"seq": peer}, device_id_type=pl.DeviceIdType.MESH,
        )

    part = lambda k: pl.ds(CHUNK * k, CHUNK)

    def z_copy(k, n, zz):
        block = qg.at[zz, y, c, part(k)]
        return remote(block, block, z_send.at[k, n - 1], z_recv.at[k, n - 1], z_peer(n))

    def y_copy(k, n, yy):
        block = qg.at[:, yy, c, part(k)]
        peer = z * NR + lax.rem(y + n, NY) * NC + c
        return remote(block, block, y_send.at[k, n - 1], y_recv.at[k, n - 1], peer)

    def c_copy(k, cc):
        block = qg.at[:, :, cc, part(k)]
        return remote(block, block, c_send.at[k], c_recv.at[k], z * NR + y * NC + 1 - c)

    def s1_copy(k, n, zz):
        block = st1.at[k, zz]
        return remote(block, block, s1_send.at[k, n - 1], s1_recv.at[k, n - 1], z_peer(n))

    def s2_copy(k, n, rr):
        block = st2.at[k, rr]
        return remote(block, block, s2_send.at[k, n - 1], s2_recv.at[k, n - 1], r_peer(n))

    def d_copy(k):
        return remote(over.at[part(k)], over_in.at[part(k)], d_send.at[k], d_recv.at[k], ahead)

    def z_to_y(k):
        for n in range(1, NZ):
            z_copy(k, n, lax.rem(z + NZ - n, NZ)).wait_recv()
        for n in range(1, NY):
            y_copy(k, n, y).start()

    def y_to_c(k):
        for n in range(1, NY):
            y_copy(k, n, lax.rem(y + NY - n, NY)).wait_recv()
        c_copy(k, c).start()

    def s1_to_s2(k):
        for n in range(1, NZ):
            s1_copy(k, n, lax.rem(z + NZ - n, NZ)).wait_recv()
        st2[k, r] = combined([st1[k, n] for n in range(NZ)])
        for n in range(1, NR):
            s2_copy(k, n, r).start()

    def queries(layer, group):
        return qg[:, :, :, layer, group].reshape(-1, HD)

    own.wait()
    pl.semaphore_wait(barrier, len(greeted))
    for k in range(chunks):
        for n in range(1, NZ):
            z_copy(k, n, z).start()
    z_to_y(0)
    z_to_y(1)
    y_to_c(0)
    key_copy(0).wait()
    c_copy(0, 1 - c).wait_recv()
    score(queries(0, 0), kv, 0, 0, sa)

    def gather_stats(k, row, m_ref, t_ref, mt_ref):
        found = row_stats(m_ref, t_ref, mt_ref)
        for half in range(2):
            st1[k, z, pl.ds(2 * row + half, 1), :] = found[:, half * LANES : half * LANES + LANES]

    def first_pass(k, carry):
        @pl.when(k + 1 < chunks)
        def _():
            y_to_c(k + 1)

        @pl.when(k + 2 < chunks)
        def _():
            z_to_y(k + 2)

        def layer_pass(j, carry):
            layer = CHUNK * k + j
            following = jnp.minimum(layer + 1, layers - 1)
            score(queries(layer, 1), kv, layer, 1, sb)
            weigh(sa, wv.at[layer, 0], mv.at[0], tv.at[0], limit)
            gather_stats(k, 2 * j, mv.at[0], tv.at[0], mt.at[layer, 0])

            @pl.when(layer + 1 < layers)
            def _():
                key_copy(layer + 1).wait()

            @pl.when((j == CHUNK - 1) & (k + 1 < chunks))
            def _():
                c_copy(k + 1, 1 - c).wait_recv()

            score(queries(following, 0), kv, following, 0, sa)
            weigh(sb, wv.at[layer, 1], mv.at[1], tv.at[1], limit)
            gather_stats(k, 2 * j + 1, mv.at[1], tv.at[1], mt.at[layer, 1])
            return carry

        lax.fori_loop(0, CHUNK, layer_pass, 0)
        for n in range(1, NZ):
            s1_copy(k, n, z).start()

        @pl.when(k > 0)
        def _():
            s1_to_s2(k - 1)

        return carry

    lax.fori_loop(0, chunks, first_pass, 0)

    def out_copies(k):
        return [
            pltpu.make_async_copy(vo.at[part(k)], vert_hbm.at[part(k)], o_sem.at[k, 0]),
            pltpu.make_async_copy(so.at[part(k)], slash_hbm.at[part(k)], o_sem.at[k, 1]),
        ]

    def finish(k):
        d_copy(k).wait_recv()
        for j in range(CHUNK):
            so[CHUNK * k + j, :, 0:LANES] = so[CHUNK * k + j, :, 0:LANES] + over_in[CHUNK * k + j]
        for copy in out_copies(k):
            copy.start()

    def second_pass(k, carry):
        for n in range(1, NR):
            s2_copy(k, n, lax.rem(r + NR - n, NR)).wait_recv()
        total[...] = math.log2(so.shape[2] * count / LAST) - combined([st2[k, n] for n in range(NR)])

        def layer_pass(j, carry):
            layer = CHUNK * k + j
            for group in range(2):
                for half in range(2):
                    at = slice(half * LANES, half * LANES + LANES)
                    offset = total[pl.ds(4 * j + 2 * group + half, 1), :]
                    fv[group, at, :] = jnp.exp2(mt[layer, group, :, at] * SCALE + offset).T
                spread(
                    wv.at[layer, group], fv.at[group],
                    vo.at[layer], so.at[layer], over.at[layer], group,
                )
            return carry

        lax.fori_loop(0, CHUNK, layer_pass, 0)
        d_copy(k).start()

        @pl.when(k == 0)
        def _():
            s1_to_s2(chunks - 1)

        @pl.when(k > 0)
        def _():
            finish(k - 1)

        return carry

    lax.fori_loop(0, chunks, second_pass, 0)
    finish(chunks - 1)

    def drain(k, carry):
        for n in range(1, NZ):
            z_copy(k, n, z).wait_send()
            s1_copy(k, n, z).wait_send()
        for n in range(1, NY):
            y_copy(k, n, y).wait_send()
        for n in range(1, NR):
            s2_copy(k, n, r).wait_send()
        c_copy(k, c).wait_send()
        d_copy(k).wait_send()
        for copy in out_copies(k):
            copy.wait()
        return carry

    lax.fori_loop(0, chunks, drain, 0)


def on_device(tail_queries, keys):
    layers, key_count, width = keys.shape
    groups = width // HD
    heads = tail_queries.shape[2] // HD
    per_group = heads // groups
    rows = LAST * per_group
    chunks = layers // CHUNK
    q = tail_queries.reshape(layers, groups, per_group, HD)
    out = jax.ShapeDtypeStruct((layers, heads, key_count), F32)
    dma = pltpu.SemaphoreType.DMA
    return pl.pallas_call(
        kernel,
        out_shape=(out, out),
        in_specs=[pl.BlockSpec(memory_space=pl.ANY)] * 2,
        out_specs=[pl.BlockSpec(memory_space=pl.ANY)] * 2,
        scratch_shapes=[
            pltpu.VMEM((NZ, NY, NC, layers, groups, per_group, HD), BF16),
            pltpu.VMEM((layers, key_count, width), BF16),
            pltpu.VMEM((rows, key_count), F32),
            pltpu.VMEM((rows, key_count), F32),
            pltpu.VMEM((layers, groups, rows, key_count), F32),
            pltpu.VMEM((groups, rows, LANES), F32),
            pltpu.VMEM((groups, rows, LANES), F32),
            pltpu.VMEM((layers, groups, LANES, rows), F32),
            pltpu.VMEM((groups, rows, LANES), F32),
            pltpu.VMEM((layers, heads, key_count), F32),
            pltpu.VMEM((layers, heads, key_count), F32),
            pltpu.VMEM((layers, heads, LANES), F32),
            pltpu.VMEM((layers, heads, LANES), F32),
            pltpu.VMEM((chunks, NZ, 8, LANES), F32),
            pltpu.VMEM((chunks, NR, 8, LANES), F32),
            pltpu.VMEM((8, LANES), F32),
            dma,
            dma((layers,)),
            dma((chunks, 2)),
            dma((chunks, NZ - 1)),
            dma((chunks, NZ - 1)),
            dma((chunks, NY - 1)),
            dma((chunks, NY - 1)),
            dma((chunks,)),
            dma((chunks,)),
            dma((chunks, NZ - 1)),
            dma((chunks, NZ - 1)),
            dma((chunks, NR - 1)),
            dma((chunks, NR - 1)),
            dma((chunks,)),
            dma((chunks,)),
        ],
        compiler_params=pltpu.CompilerParams(
            collective_id=0, has_side_effects=True, vmem_limit_bytes=67043328
        ),
    )(q, keys)


def solution(mesh):
    return jax.shard_map(
        on_device,
        mesh=mesh,
        in_specs=(P(None, "seq", "head"), P(None, "seq", "head")),
        out_specs=(P(None, "head", "seq"), P(None, "head", "seq")),
        check_vma=False,
    )
```

```python
import functools
import math

import jax
import jax.numpy as jnp
from jax import lax
from jax.experimental import pallas as pl
from jax.experimental.pallas import tpu as pltpu
from jax.sharding import PartitionSpec as P

HD = 128
LAST = 64
LANES = 128
F32 = jnp.float32
BF16 = jnp.bfloat16
SCALE = math.log2(math.e) / math.sqrt(HD)
CHUNK = 2
NZ, NY, NC = 8, 4, 2
NR = NY * NC
TILES = 16
TAUS = TILES + LAST // 2 - 1
BIASES = 2 * TILES


def tree(op, xs):
    xs = list(xs)
    while len(xs) > 1:
        xs = [op(*xs[n : n + 2]) if n + 1 < len(xs) else xs[n] for n in range(0, len(xs), 2)]
    return xs[0]


def combined(parts):
    top = tree(jnp.maximum, parts)
    return top + jnp.log2(tree(jnp.add, [jnp.exp2(part - top) for part in parts]))


def score(q, k_ref, layer, group, s_ref):
    for n in range(0, TILES, 2):
        tile = lambda m: k_ref[layer, m % 4, :, m // 4, :, HD * group : HD * group + HD].reshape(LANES, HD)
        k = jnp.concatenate([tile(n), tile(n + 1)], axis=0)
        s_ref[:, n * LANES : (n + 2) * LANES] = lax.dot_general(
            q, k, (((1,), (1,)), ((), ())), preferred_element_type=F32
        )


def iotas():
    return tuple(lax.broadcasted_iota(jnp.int32, (8, LANES), dim) for dim in range(2))


def fill_bias(bias_ref, limit):
    sub, lane = iotas()
    key = 32 * (lane >> 1) + (lane & 1) - (sub >> 2)
    for d in range(BIASES):
        bias_ref[d] = jnp.where(key > limit + 2 * (d - TILES + 1), -1e30, 0.0)


def weigh(s_ref, w_ref, m_ref, t_ref, bias_ref):
    for v in range(s_ref.shape[0] // 8):
        at = slice(8 * v, 8 * v + 8)
        xs = []
        for n in range(TILES):
            x = s_ref[at, n * LANES : n * LANES + LANES]
            d = v - n + TILES - 1
            xs.append(x + bias_ref[d] if d < BIASES else x)
        top = tree(jnp.maximum, xs)
        ws = [jnp.exp2((x - top) * SCALE) for x in xs]
        for n, w in enumerate(ws):
            w_ref[at, n * LANES : n * LANES + LANES] = w
        m_ref[at, :] = top
        t_ref[at, :] = tree(jnp.add, ws)


def row_stats(m_ref, t_ref, mt_ref):
    mt = m_ref[...].T
    mt_ref[...] = mt
    top = jnp.max(mt, axis=0, keepdims=True)
    total = jnp.sum(t_ref[...].T * jnp.exp2((mt - top) * SCALE), axis=0, keepdims=True)
    return top * SCALE + jnp.log2(total)


def accumulate(w_ref, f_ref, acc_ref):
    groups = w_ref.shape[0] // 8
    vert = [None] * TILES
    diag = [None] * TAUS
    add = lambda a, b: b if a is None else a + b
    for v in range(groups):
        at = slice(8 * v, 8 * v + 8)
        factor = f_ref[at, :]
        start = groups - 1 - v
        for n in range(TILES):
            p = w_ref[at, n * LANES : n * LANES + LANES] * factor
            vert[n] = add(vert[n], p)
            diag[start + n] = add(diag[start + n], p)
        acc_ref[start + TILES - 1] = diag[start + TILES - 1]
    for t in range(TILES - 1):
        acc_ref[t] = diag[t]
    for n in range(TILES):
        acc_ref[TAUS + n] = vert[n]


def natural(tiles):
    _, lane = iotas()
    turned = [tiles[0]] + [pltpu.roll(tiles[n], 8 * n, 1) for n in range(1, TILES)]
    turned = [turned[-n] for n in range(TILES)]
    for bit in range(4):
        step = ((lane >> (3 + bit)) & 1) == 1
        turned = [jnp.where(step, turned[n - (1 << bit)], turned[n]) for n in range(TILES)]
    return [interleaved(x, 8 * n) for n, x in enumerate(turned)]


def interleaved(x, start=0):
    _, lane = iotas()
    source = (start + ((lane >> 1) & 15) * 8 + (lane >> 5) * 2 + (lane & 1)) & (LANES - 1)
    return jnp.take_along_axis(x, source, axis=1)


def both(first, second):
    sub, _ = iotas()
    return jnp.where(sub < 4, first, second)


def folded(x):
    return x + pltpu.roll(x, 4, 0)


def whole_lanes(acc_ref):
    _, lane = iotas()
    inside, outside = [], []
    for n in range(TILES):
        x, y = acc_ref[n], None
        for c in range(1, 3):
            if TILES * c + n < TAUS:
                turned = pltpu.roll(acc_ref[TILES * c + n], 2 * c, 1)
                x = x + jnp.where(lane >= 2 * c, turned, 0.0)
                past = jnp.where(lane < 2 * c, turned, 0.0)
                y = past if y is None else y + past
        inside.append(x)
        outside.append(y)
    return inside, outside


def settle(acc_refs):
    _, lane = iotas()
    odd = (lane & 1) == 1
    turn = lambda x: pltpu.roll(x, 4, 0)
    (in0, out0), (in1, out1) = (whole_lanes(acc_ref) for acc_ref in acc_refs)
    upper = lambda xs, ys: [both(x, turn(y)) for x, y in zip(xs, ys)]
    lower = lambda xs, ys: [both(turn(x), y) for x, y in zip(xs, ys)]
    late, same = upper(in0, in1), lower(in0, in1)
    last = pltpu.roll(late[-1], 1, 1)
    overs = []
    for past in (upper(out0, out1), lower(out0, out1)):
        past = [past[0]] + [pltpu.roll(past[n], 8 * n, 1) for n in range(1, TILES)]
        overs.append(interleaved(tree(jnp.add, past)))
    over = jnp.where(lane < 1, last, pltpu.roll(overs[0], 1, 1)) + overs[1]

    def ordered():
        up = [pltpu.roll(x, 1, 1) for x in late[:-1]]
        down = [pltpu.roll(x, LANES - 1, 1) for x in late[:-1]]
        up.append(last)
        moved = [jnp.where(odd, up[0], jnp.where(lane < 1, 0.0, last))]
        moved += [jnp.where(odd, up[n], down[n - 1]) for n in range(1, TILES)]
        slash = natural([x + y for x, y in zip(moved, same)])
        vert = natural([both(*(folded(acc_ref[TAUS + n]) for acc_ref in acc_refs)) for n in range(TILES)])
        return vert, slash

    return over, ordered


def kernel(
    q_hbm, k_hbm, vo, so,
    qv, qg, kv, sa, sb, wv, mv, tv, mt, fv, acc, bias, over, over_in, st1, st2, total,
    q_sem, k_sem,
    z_send, z_recv, y_send, y_recv, c_send, c_recv,
    s1_send, s1_recv, s2_send, s2_recv, d_send, d_recv,
):
    layers = kv.shape[0]
    chunks = layers // CHUNK
    seq = lax.axis_index("seq")
    z, r = seq // NR, lax.rem(seq, NR)
    y, c = r // NC, lax.rem(r, NC)
    z_peer = lambda n: lax.rem(z + n, NZ) * NR + r
    r_peer = lambda n: z * NR + lax.rem(r + n, NR)
    ahead, behind = lax.rem(seq + 1, NZ * NR), lax.rem(seq + NZ * NR - 1, NZ * NR)
    count = lax.axis_size("seq")
    limit = so.shape[2] - LAST + jnp.where(seq == count - 1, 0, 1 << 20)

    own = pltpu.make_async_copy(q_hbm, qv, q_sem)
    own.start()

    def key_copies(layer, carry):
        rows = k_hbm.at[layer].reshape(8, 8, 4, 8, k_hbm.shape[2])
        for low in range(4):
            for m in range(8):
                pltpu.make_async_copy(
                    rows.at[:, m, :, pl.ds(2 * low, 2), :],
                    kv.at[layer, low, :, :, pl.ds(2 * m, 2), :],
                    k_sem.at[layer],
                ).start()
        return carry

    def keys_here(layer):
        pltpu.make_async_copy(kv.at[layer], kv.at[layer], k_sem.at[layer]).wait()

    barrier = pltpu.get_barrier_semaphore()
    greeted = [z_peer(n) for n in range(1, NZ)] + [r_peer(n) for n in range(1, NR)] + [ahead, behind]
    for peer in greeted:
        pl.semaphore_signal(barrier, inc=1, device_id={"seq": peer}, device_id_type=pl.DeviceIdType.MESH)

    def remote(src, dst, send, recv, peer):
        return pltpu.make_async_remote_copy(
            src_ref=src, dst_ref=dst, send_sem=send, recv_sem=recv,
            device_id={"seq": peer}, device_id_type=pl.DeviceIdType.MESH,
        )

    part = lambda k: pl.ds(CHUNK * k, CHUNK)

    def z_copy(k, n, zz):
        block = qg.at[zz, y, c, part(k)]
        return remote(block, block, z_send.at[k, n - 1], z_recv.at[k, n - 1], z_peer(n))

    def y_copy(k, n, yy):
        block = qg.at[:, yy, c, part(k)]
        peer = z * NR + lax.rem(y + n, NY) * NC + c
        return remote(block, block, y_send.at[k, n - 1], y_recv.at[k, n - 1], peer)

    def c_copy(k, cc):
        block = qg.at[:, :, cc, part(k)]
        return remote(block, block, c_send.at[k], c_recv.at[k], z * NR + y * NC + 1 - c)

    def s1_copy(k, n, zz):
        block = st1.at[k, zz]
        return remote(block, block, s1_send.at[k, n - 1], s1_recv.at[k, n - 1], z_peer(n))

    def s2_copy(k, n, rr):
        block = st2.at[k, rr]
        return remote(block, block, s2_send.at[k, n - 1], s2_recv.at[k, n - 1], r_peer(n))

    def d_copy(k):
        return remote(over.at[part(k)], over_in.at[part(k)], d_send.at[k], d_recv.at[k], ahead)

    def z_to_y(k):
        for n in range(1, NZ):
            z_copy(k, n, lax.rem(z + NZ - n, NZ)).wait_recv()
        for n in range(1, NY):
            y_copy(k, n, y).start()

    def y_to_c(k):
        for n in range(1, NY):
            y_copy(k, n, lax.rem(y + NY - n, NY)).wait_recv()
        c_copy(k, c).start()

    def s1_to_s2(k):
        for n in range(1, NZ):
            s1_copy(k, n, lax.rem(z + NZ - n, NZ)).wait_recv()
        st2[k, r] = combined([st1[k, n] for n in range(NZ)])
        for n in range(1, NR):
            s2_copy(k, n, r).start()

    def queries(layer, group):
        return qg[:, :, :, layer, group].reshape(-1, HD)

    lax.fori_loop(0, CHUNK, key_copies, 0)
    own.wait()
    block = qv[...].astype(F32).reshape(layers, -1, HD).astype(BF16)
    qg[z, y, c] = block.reshape(qg.shape[3:])
    fill_bias(bias, limit)
    pl.semaphore_wait(barrier, len(greeted))
    for k in range(chunks):
        for n in range(1, NZ):
            z_copy(k, n, z).start()
    lax.fori_loop(CHUNK, layers, key_copies, 0)
    z_to_y(0)
    z_to_y(1)
    y_to_c(0)
    keys_here(0)
    c_copy(0, 1 - c).wait_recv()
    score(queries(0, 0), kv, 0, 0, sa)

    def gather_stats(k, row, m_ref, t_ref, mt_ref):
        found = row_stats(m_ref, t_ref, mt_ref)
        for half in range(2):
            st1[k, z, pl.ds(2 * row + half, 1), :] = found[:, half * LANES : half * LANES + LANES]

    def first_pass(k, carry):
        @pl.when(k + 1 < chunks)
        def _():
            y_to_c(k + 1)

        @pl.when(k + 2 < chunks)
        def _():
            z_to_y(k + 2)

        def layer_pass(j, carry):
            layer = CHUNK * k + j
            following = jnp.minimum(layer + 1, layers - 1)
            score(queries(layer, 1), kv, layer, 1, sb)
            weigh(sa, wv.at[layer, 0], mv.at[0], tv.at[0], bias)
            gather_stats(k, 2 * j, mv.at[0], tv.at[0], mt.at[layer, 0])

            @pl.when(layer + 1 < layers)
            def _():
                keys_here(layer + 1)

            @pl.when((j == CHUNK - 1) & (k + 1 < chunks))
            def _():
                c_copy(k + 1, 1 - c).wait_recv()

            score(queries(following, 0), kv, following, 0, sa)
            weigh(sb, wv.at[layer, 1], mv.at[1], tv.at[1], bias)
            gather_stats(k, 2 * j + 1, mv.at[1], tv.at[1], mt.at[layer, 1])
            return carry

        lax.fori_loop(0, CHUNK, layer_pass, 0)
        for n in range(1, NZ):
            s1_copy(k, n, z).start()

        @pl.when(k > 0)
        def _():
            s1_to_s2(k - 1)

        return carry

    lax.fori_loop(0, chunks, first_pass, 0)

    def finish(k):
        d_copy(k).wait_recv()
        for j in range(CHUNK):
            so[CHUNK * k + j, :, 0:LANES] = so[CHUNK * k + j, :, 0:LANES] + over_in[CHUNK * k + j]

    def second_pass(k, carry):
        for n in range(1, NR):
            s2_copy(k, n, lax.rem(r + NR - n, NR)).wait_recv()
        total[...] = math.log2(so.shape[2] * count / LAST) - combined([st2[k, n] for n in range(NR)])
        for j in range(CHUNK):
            for group in range(2):
                for half in range(2):
                    at = slice(half * LANES, half * LANES + LANES)
                    row = 4 * j + 2 * group + half
                    logs = mt[CHUNK * k + j, group, :, at] * SCALE + total[row : row + 1, :]
                    fv[j, group, at, :] = jnp.exp2(logs).T

        def sums(n, carry):
            j, group = n // 2, lax.rem(n, 2)
            accumulate(wv.at[CHUNK * k + j, group], fv.at[j, group], acc.at[j, group])
            return carry

        lax.fori_loop(0, 2 * CHUNK, sums, 0)
        rest = []
        for j in range(CHUNK):
            over[CHUNK * k + j], ordered = settle([acc.at[j, 0], acc.at[j, 1]])
            rest.append(ordered)
        d_copy(k).start()
        for j in range(CHUNK):
            for ref, tiles in zip((vo, so), rest[j]()):
                for n in range(TILES):
                    ref[CHUNK * k + j, :, n * LANES : n * LANES + LANES] = tiles[n]

        @pl.when(k == 0)
        def _():
            s1_to_s2(chunks - 1)

        @pl.when(k > 0)
        def _():
            finish(k - 1)

        return carry

    lax.fori_loop(0, chunks, second_pass, 0)
    finish(chunks - 1)

    def drain(k, carry):
        for n in range(1, NZ):
            z_copy(k, n, z).wait_send()
            s1_copy(k, n, z).wait_send()
        for n in range(1, NY):
            y_copy(k, n, y).wait_send()
        for n in range(1, NR):
            s2_copy(k, n, r).wait_send()
        c_copy(k, c).wait_send()
        d_copy(k).wait_send()
        return carry

    lax.fori_loop(0, chunks, drain, 0)


def on_device(tail_queries, keys):
    layers, key_count, width = keys.shape
    groups = width // HD
    heads = tail_queries.shape[2] // HD
    per_group = heads // groups
    rows = LAST * per_group
    chunks = layers // CHUNK
    q = tail_queries.reshape(layers, heads * HD)
    out = jax.ShapeDtypeStruct((layers, heads, key_count), F32)
    dma = pltpu.SemaphoreType.DMA
    return pl.pallas_call(
        kernel,
        out_shape=(out, out),
        in_specs=[pl.BlockSpec(memory_space=pl.ANY)] * 2,
        out_specs=[pl.BlockSpec(memory_space=pltpu.VMEM)] * 2,
        scratch_shapes=[
            pltpu.VMEM((layers, heads * HD), BF16),
            pltpu.VMEM((NZ, NY, NC, layers, groups, per_group, HD), BF16),
            pltpu.VMEM((layers, 4, 8, 4, 16, width), BF16),
            pltpu.VMEM((rows, key_count), F32),
            pltpu.VMEM((rows, key_count), F32),
            pltpu.VMEM((layers, groups, rows, key_count), F32),
            pltpu.VMEM((groups, rows, LANES), F32),
            pltpu.VMEM((groups, rows, LANES), F32),
            pltpu.VMEM((layers, groups, LANES, rows), F32),
            pltpu.VMEM((CHUNK, groups, rows, LANES), F32),
            pltpu.VMEM((CHUNK, groups, TAUS + TILES, 8, LANES), F32),
            pltpu.VMEM((BIASES, 8, LANES), F32),
            pltpu.VMEM((layers, heads, LANES), F32),
            pltpu.VMEM((layers, heads, LANES), F32),
            pltpu.VMEM((chunks, NZ, 8, LANES), F32),
            pltpu.VMEM((chunks, NR, 8, LANES), F32),
            pltpu.VMEM((8, LANES), F32),
            dma,
            dma((layers,)),
            dma((chunks, NZ - 1)),
            dma((chunks, NZ - 1)),
            dma((chunks, NY - 1)),
            dma((chunks, NY - 1)),
            dma((chunks,)),
            dma((chunks,)),
            dma((chunks, NZ - 1)),
            dma((chunks, NZ - 1)),
            dma((chunks, NR - 1)),
            dma((chunks, NR - 1)),
            dma((chunks,)),
            dma((chunks,)),
        ],
        compiler_params=pltpu.CompilerParams(
            collective_id=0, has_side_effects=True, vmem_limit_bytes=65900000
        ),
    )(q, keys)


def solution(mesh):
    return jax.shard_map(
        on_device,
        mesh=mesh,
        in_specs=(P(None, "seq", "head"), P(None, "seq", "head")),
        out_specs=(P(None, "head", "seq"), P(None, "head", "seq")),
        check_vma=False,
    )
```

```python
import functools
import math

import jax
import jax.numpy as jnp
from jax import lax
from jax.experimental import pallas as pl
from jax.experimental.pallas import tpu as pltpu
from jax.sharding import PartitionSpec as P

HD = 128
LAST = 64
LANES = 128
F32 = jnp.float32
BF16 = jnp.bfloat16
SCALE = math.log2(math.e) / math.sqrt(HD)
CHUNK = 2
NZ, NY, NC = 8, 4, 2
NR = NY * NC
TILES = 16
TAUS = TILES + LAST // 2 - 1
BIASES = 2 * TILES


def tree(op, xs):
    xs = list(xs)
    while len(xs) > 1:
        xs = [op(*xs[n : n + 2]) if n + 1 < len(xs) else xs[n] for n in range(0, len(xs), 2)]
    return xs[0]


def combined(parts):
    top = tree(jnp.maximum, parts)
    return top + jnp.log2(tree(jnp.add, [jnp.exp2(part - top) for part in parts]))


def score(q, k_ref, layer, group, s_ref):
    for n in range(0, TILES, 2):
        tile = lambda m: k_ref[layer, m % 4, :, m // 4, :, HD * group : HD * group + HD].reshape(LANES, HD)
        k = jnp.concatenate([tile(n), tile(n + 1)], axis=0)
        s_ref[:, n * LANES : (n + 2) * LANES] = lax.dot_general(
            q, k, (((1,), (1,)), ((), ())), preferred_element_type=F32
        )


def iotas():
    return tuple(lax.broadcasted_iota(jnp.int32, (8, LANES), dim) for dim in range(2))


def fill_bias(bias_ref, limit):
    sub, lane = iotas()
    key = 32 * (lane >> 1) + (lane & 1) - (sub >> 2)
    for d in range(BIASES):
        bias_ref[d] = jnp.where(key > limit + 2 * (d - TILES + 1), -1e30, 0.0)


def weigh(s_ref, w_ref, m_ref, t_ref, bias_ref):
    for v in range(s_ref.shape[0] // 8):
        at = slice(8 * v, 8 * v + 8)
        xs = []
        for n in range(TILES):
            x = s_ref[at, n * LANES : n * LANES + LANES]
            d = v - n + TILES - 1
            xs.append(x + bias_ref[d] if d < BIASES else x)
        top = tree(jnp.maximum, xs)
        ws = [jnp.exp2((x - top) * SCALE) for x in xs]
        for n, w in enumerate(ws):
            w_ref[at, n * LANES : n * LANES + LANES] = w
        m_ref[at, :] = top
        t_ref[at, :] = tree(jnp.add, ws)


def row_stats(m_ref, t_ref, mt_ref):
    mt = m_ref[...].T
    mt_ref[...] = mt
    top = jnp.max(mt, axis=0, keepdims=True)
    total = jnp.sum(t_ref[...].T * jnp.exp2((mt - top) * SCALE), axis=0, keepdims=True)
    return top * SCALE + jnp.log2(total)


def accumulate(w_ref, f_ref, acc_ref):
    groups = w_ref.shape[0] // 8
    vert = [None] * TILES
    diag = [None] * TAUS
    add = lambda a, b: b if a is None else a + b
    for v in range(groups):
        at = slice(8 * v, 8 * v + 8)
        factor = f_ref[at, :]
        start = groups - 1 - v
        for n in range(TILES):
            p = w_ref[at, n * LANES : n * LANES + LANES] * factor
            vert[n] = add(vert[n], p)
            diag[start + n] = add(diag[start + n], p)
        acc_ref[start + TILES - 1] = diag[start + TILES - 1]
    for t in range(TILES - 1):
        acc_ref[t] = diag[t]
    for n in range(TILES):
        acc_ref[TAUS + n] = vert[n]


def natural(tiles):
    _, lane = iotas()
    turned = [tiles[0]] + [pltpu.roll(tiles[n], 8 * n, 1) for n in range(1, TILES)]
    turned = [turned[-n] for n in range(TILES)]
    for bit in range(4):
        step = ((lane >> (3 + bit)) & 1) == 1
        turned = [jnp.where(step, turned[n - (1 << bit)], turned[n]) for n in range(TILES)]
    return [interleaved(x, 8 * n) for n, x in enumerate(turned)]


def interleaved(x, start=0):
    _, lane = iotas()
    source = (start + ((lane >> 1) & 15) * 8 + (lane >> 5) * 2 + (lane & 1)) & (LANES - 1)
    return jnp.take_along_axis(x, source, axis=1)


def both(first, second):
    sub, _ = iotas()
    return jnp.where(sub < 4, first, second)


def folded(x):
    return x + pltpu.roll(x, 4, 0)


def whole_lanes(acc_ref):
    _, lane = iotas()
    inside, outside = [], []
    for n in range(TILES):
        x, y = acc_ref[n], None
        for c in range(1, 3):
            if TILES * c + n < TAUS:
                turned = pltpu.roll(acc_ref[TILES * c + n], 2 * c, 1)
                x = x + jnp.where(lane >= 2 * c, turned, 0.0)
                past = jnp.where(lane < 2 * c, turned, 0.0)
                y = past if y is None else y + past
        inside.append(x)
        outside.append(y)
    return inside, outside


def settle(acc_refs):
    _, lane = iotas()
    odd = (lane & 1) == 1
    turn = lambda x: pltpu.roll(x, 4, 0)
    (in0, out0), (in1, out1) = (whole_lanes(acc_ref) for acc_ref in acc_refs)
    upper = lambda xs, ys: [both(x, turn(y)) for x, y in zip(xs, ys)]
    lower = lambda xs, ys: [both(turn(x), y) for x, y in zip(xs, ys)]
    late, same = upper(in0, in1), lower(in0, in1)
    last = pltpu.roll(late[-1], 1, 1)
    overs = []
    for past in (upper(out0, out1), lower(out0, out1)):
        past = [past[0]] + [pltpu.roll(past[n], 8 * n, 1) for n in range(1, TILES)]
        overs.append(interleaved(tree(jnp.add, past)))
    over = jnp.where(lane < 1, last, pltpu.roll(overs[0], 1, 1)) + overs[1]

    def ordered():
        up = [pltpu.roll(x, 1, 1) for x in late[:-1]]
        down = [pltpu.roll(x, LANES - 1, 1) for x in late[:-1]]
        up.append(last)
        moved = [jnp.where(odd, up[0], jnp.where(lane < 1, 0.0, last))]
        moved += [jnp.where(odd, up[n], down[n - 1]) for n in range(1, TILES)]
        slash = natural([x + y for x, y in zip(moved, same)])
        vert = natural([both(*(folded(acc_ref[TAUS + n]) for acc_ref in acc_refs)) for n in range(TILES)])
        return vert, slash

    return over, ordered


def kernel(
    q_hbm, k_hbm, vo, so,
    qv, qg, kv, sa, sb, wv, mv, tv, mt, fv, acc, bias, over, over_in, st1, st2, total,
    q_sem, k_sem,
    z_send, z_recv, y_send, y_recv, c_send, c_recv,
    s1_send, s1_recv, s2_send, s2_recv, d_send, d_recv,
):
    layers = kv.shape[0]
    chunks = layers // CHUNK
    seq = lax.axis_index("seq")
    z, r = seq // NR, lax.rem(seq, NR)
    y, c = r // NC, lax.rem(r, NC)
    z_peer = lambda n: lax.rem(z + n, NZ) * NR + r
    r_peer = lambda n: z * NR + lax.rem(r + n, NR)
    ahead, behind = lax.rem(seq + 1, NZ * NR), lax.rem(seq + NZ * NR - 1, NZ * NR)
    count = lax.axis_size("seq")
    limit = so.shape[2] - LAST + jnp.where(seq == count - 1, 0, 1 << 20)

    own = pltpu.make_async_copy(q_hbm, qv, q_sem)
    own.start()

    def key_copies(layer, carry):
        rows = k_hbm.at[layer].reshape(8, 8, 4, 8, k_hbm.shape[2])
        for low in range(4):
            for m in range(8):
                pltpu.make_async_copy(
                    rows.at[:, m, :, pl.ds(2 * low, 2), :],
                    kv.at[layer, low, :, :, pl.ds(2 * m, 2), :],
                    k_sem.at[layer],
                ).start()
        return carry

    def keys_here(layer):
        pltpu.make_async_copy(kv.at[layer], kv.at[layer], k_sem.at[layer]).wait()

    barrier = pltpu.get_barrier_semaphore()
    greeted = [z_peer(n) for n in range(1, NZ)] + [r_peer(n) for n in range(1, NR)] + [ahead, behind]
    for peer in greeted:
        pl.semaphore_signal(barrier, inc=1, device_id={"seq": peer}, device_id_type=pl.DeviceIdType.MESH)

    def remote(src, dst, send, recv, peer):
        return pltpu.make_async_remote_copy(
            src_ref=src, dst_ref=dst, send_sem=send, recv_sem=recv,
            device_id={"seq": peer}, device_id_type=pl.DeviceIdType.MESH,
        )

    part = lambda k: pl.ds(CHUNK * k, CHUNK)

    def z_copy(k, n, zz):
        block = qg.at[zz, y, c, k]
        return remote(block, block, z_send.at[k, n - 1], z_recv.at[k, n - 1], z_peer(n))

    def y_copy(k, n, yy):
        block = qg.at[:, yy, c, k]
        peer = z * NR + lax.rem(y + n, NY) * NC + c
        return remote(block, block, y_send.at[k, n - 1], y_recv.at[k, n - 1], peer)

    def c_copy(k, cc):
        block = qg.at[:, :, cc, k]
        return remote(block, block, c_send.at[k], c_recv.at[k], z * NR + y * NC + 1 - c)

    def s1_copy(k, n, zz):
        block = st1.at[k, zz]
        return remote(block, block, s1_send.at[k, n - 1], s1_recv.at[k, n - 1], z_peer(n))

    def s2_copy(k, n, rr):
        block = st2.at[k, rr]
        return remote(block, block, s2_send.at[k, n - 1], s2_recv.at[k, n - 1], r_peer(n))

    def d_copy(k):
        return remote(over.at[part(k)], over_in.at[part(k)], d_send.at[k], d_recv.at[k], ahead)

    def z_to_y(k):
        for n in range(1, NZ):
            z_copy(k, n, lax.rem(z + NZ - n, NZ)).wait_recv()
        for n in range(1, NY):
            y_copy(k, n, y).start()

    def y_to_c(k):
        for n in range(1, NY):
            y_copy(k, n, lax.rem(y + NY - n, NY)).wait_recv()
        c_copy(k, c).start()

    def s1_to_s2(k):
        for n in range(1, NZ):
            s1_copy(k, n, lax.rem(z + NZ - n, NZ)).wait_recv()
        st2[k, r] = combined([st1[k, n] for n in range(NZ)])
        for n in range(1, NR):
            s2_copy(k, n, r).start()

    def queries(layer, group):
        return qg[:, :, :, layer, group].reshape(-1, HD)

    lax.fori_loop(0, CHUNK, key_copies, 0)
    own.wait()
    block = qv[...].astype(F32).reshape(layers, -1, HD).astype(BF16)
    qg[z, y, c] = block.reshape(qg.shape[3:])
    fill_bias(bias, limit)
    pl.semaphore_wait(barrier, len(greeted))
    def z_starts(k, carry):
        for n in range(1, NZ):
            z_copy(k, n, z).start()
        return carry

    lax.fori_loop(0, layers, z_starts, 0)
    lax.fori_loop(CHUNK, layers, key_copies, 0)

    def z_passes(k, carry):
        z_to_y(k)
        return carry

    lax.fori_loop(0, layers, z_passes, 0)
    y_to_c(0)
    y_to_c(1)
    keys_here(0)
    c_copy(0, 1 - c).wait_recv()
    score(queries(0, 0), kv, 0, 0, sa)

    def gather_stats(k, row, m_ref, t_ref, mt_ref):
        found = row_stats(m_ref, t_ref, mt_ref)
        for half in range(2):
            st1[k, z, pl.ds(2 * row + half, 1), :] = found[:, half * LANES : half * LANES + LANES]

    def first_pass(k, carry):
        def layer_pass(j, carry):
            layer = CHUNK * k + j
            following = jnp.minimum(layer + 1, layers - 1)
            score(queries(layer, 1), kv, layer, 1, sb)
            weigh(sa, wv.at[layer, 0], mv.at[0], tv.at[0], bias)
            gather_stats(k, 2 * j, mv.at[0], tv.at[0], mt.at[layer, 0])

            @pl.when(layer + 2 < layers)
            def _():
                y_to_c(layer + 2)

            @pl.when(layer + 1 < layers)
            def _():
                keys_here(layer + 1)
                c_copy(layer + 1, 1 - c).wait_recv()

            score(queries(following, 0), kv, following, 0, sa)
            weigh(sb, wv.at[layer, 1], mv.at[1], tv.at[1], bias)
            gather_stats(k, 2 * j + 1, mv.at[1], tv.at[1], mt.at[layer, 1])
            return carry

        lax.fori_loop(0, CHUNK, layer_pass, 0)
        for n in range(1, NZ):
            s1_copy(k, n, z).start()

        @pl.when(k > 1)
        def _():
            s1_to_s2(k - 2)

        return carry

    lax.fori_loop(0, chunks, first_pass, 0)

    def finish(k):
        d_copy(k).wait_recv()
        for j in range(CHUNK):
            so[CHUNK * k + j, :, 0:LANES] = so[CHUNK * k + j, :, 0:LANES] + over_in[CHUNK * k + j]

    def second_pass(k, carry):
        for n in range(1, NR):
            s2_copy(k, n, lax.rem(r + NR - n, NR)).wait_recv()
        total[...] = math.log2(so.shape[2] * count / LAST) - combined([st2[k, n] for n in range(NR)])
        for j in range(CHUNK):
            for group in range(2):
                for half in range(2):
                    at = slice(half * LANES, half * LANES + LANES)
                    row = 4 * j + 2 * group + half
                    logs = mt[CHUNK * k + j, group, :, at] * SCALE + total[row : row + 1, :]
                    fv[j, group, at, :] = jnp.exp2(logs).T

        def sums(n, carry):
            j, group = n // 2, lax.rem(n, 2)
            accumulate(wv.at[CHUNK * k + j, group], fv.at[j, group], acc.at[j, group])
            return carry

        lax.fori_loop(0, 2 * CHUNK, sums, 0)
        rest = []
        for j in range(CHUNK):
            over[CHUNK * k + j], ordered = settle([acc.at[j, 0], acc.at[j, 1]])
            rest.append(ordered)
        d_copy(k).start()
        for j in range(CHUNK):
            for ref, tiles in zip((vo, so), rest[j]()):
                for n in range(TILES):
                    ref[CHUNK * k + j, :, n * LANES : n * LANES + LANES] = tiles[n]

        @pl.when(k < 2)
        def _():
            s1_to_s2(chunks - 2 + k)

        @pl.when(k > 1)
        def _():
            finish(k - 2)

        return carry

    lax.fori_loop(0, chunks, second_pass, 0)
    finish(chunks - 2)
    finish(chunks - 1)

    def drain(k, carry):
        for n in range(1, NZ):
            z_copy(k, n, z).wait_send()
        for n in range(1, NY):
            y_copy(k, n, y).wait_send()
        c_copy(k, c).wait_send()
        return carry

    def drain_stats(k, carry):
        for n in range(1, NZ):
            s1_copy(k, n, z).wait_send()
        for n in range(1, NR):
            s2_copy(k, n, r).wait_send()
        d_copy(k).wait_send()
        return carry

    lax.fori_loop(0, layers, drain, 0)
    lax.fori_loop(0, chunks, drain_stats, 0)


def on_device(tail_queries, keys):
    layers, key_count, width = keys.shape
    groups = width // HD
    heads = tail_queries.shape[2] // HD
    per_group = heads // groups
    rows = LAST * per_group
    chunks = layers // CHUNK
    q = tail_queries.reshape(layers, heads * HD)
    out = pltpu.VMEM((layers, heads, key_count), F32)
    dma = pltpu.SemaphoreType.DMA
    return pl.pallas_call(
        kernel,
        out_shape=(out, out),
        in_specs=[pl.BlockSpec(memory_space=pl.ANY)] * 2,
        out_specs=[pl.BlockSpec(memory_space=pltpu.VMEM)] * 2,
        scratch_shapes=[
            pltpu.VMEM((layers, heads * HD), BF16),
            pltpu.VMEM((NZ, NY, NC, layers, groups, per_group, HD), BF16),
            pltpu.VMEM((layers, 4, 8, 4, 16, width), BF16),
            pltpu.VMEM((rows, key_count), F32),
            pltpu.VMEM((rows, key_count), F32),
            pltpu.VMEM((layers, groups, rows, key_count), F32),
            pltpu.VMEM((groups, rows, LANES), F32),
            pltpu.VMEM((groups, rows, LANES), F32),
            pltpu.VMEM((layers, groups, LANES, rows), F32),
            pltpu.VMEM((CHUNK, groups, rows, LANES), F32),
            pltpu.VMEM((CHUNK, groups, TAUS + TILES, 8, LANES), F32),
            pltpu.VMEM((BIASES, 8, LANES), F32),
            pltpu.VMEM((layers, heads, LANES), F32),
            pltpu.VMEM((layers, heads, LANES), F32),
            pltpu.VMEM((chunks, NZ, 8, LANES), F32),
            pltpu.VMEM((chunks, NR, 8, LANES), F32),
            pltpu.VMEM((8, LANES), F32),
            dma,
            dma((layers,)),
            dma((layers, NZ - 1)),
            dma((layers, NZ - 1)),
            dma((layers, NY - 1)),
            dma((layers, NY - 1)),
            dma((layers,)),
            dma((layers,)),
            dma((chunks, NZ - 1)),
            dma((chunks, NZ - 1)),
            dma((chunks, NR - 1)),
            dma((chunks, NR - 1)),
            dma((chunks,)),
            dma((chunks,)),
        ],
        compiler_params=pltpu.CompilerParams(
            collective_id=0, has_side_effects=True, vmem_limit_bytes=64600000
        ),
    )(q, keys)


def solution(mesh):
    return jax.shard_map(
        on_device,
        mesh=mesh,
        in_specs=(P(None, "seq", "head"), P(None, "seq", "head")),
        out_specs=(P(None, "head", "seq"), P(None, "head", "seq")),
        check_vma=False,
    )
```

```python
import functools
import math

import jax
import jax.numpy as jnp
from jax import lax
from jax.experimental import pallas as pl
from jax.experimental.pallas import tpu as pltpu
from jax.sharding import PartitionSpec as P

HD = 128
LAST = 64
LANES = 128
F32 = jnp.float32
BF16 = jnp.bfloat16
SCALE = math.log2(math.e) / math.sqrt(HD)
CHUNK = 2
NZ, NY, NC = 8, 4, 2
NR = NY * NC
TILES = 16
TAUS = TILES + LAST // 2 - 1
BIASES = 2 * TILES


def tree(op, xs):
    xs = list(xs)
    while len(xs) > 1:
        xs = [op(*xs[n : n + 2]) if n + 1 < len(xs) else xs[n] for n in range(0, len(xs), 2)]
    return xs[0]


def combined(parts):
    top = tree(jnp.maximum, parts)
    return top + jnp.log2(tree(jnp.add, [jnp.exp2(part - top) for part in parts]))


def score(q, k_ref, layer, group, s_ref, m_ref, bias_ref):
    tile = lambda n: k_ref[layer, n % 4, :, n // 4, :, HD * group : HD * group + HD].reshape(LANES, HD)
    for n in range(0, TILES, 4):
        k = jnp.concatenate([tile(n + i) for i in range(4)], axis=0)
        x = lax.dot_general(q, k, (((1,), (1,)), ((), ())), preferred_element_type=F32)
        for v in range(q.shape[0] // 8):
            at = slice(8 * v, 8 * v + 8)
            tops = [m_ref[at, :]] if n else []
            for i in range(4):
                y = x[at, i * LANES : i * LANES + LANES]
                d = v - n - i + TILES - 1
                if d < BIASES:
                    y = y + bias_ref[d]
                s_ref[at, (n + i) * LANES : (n + i + 1) * LANES] = y
                tops.append(y)
            m_ref[at, :] = tree(jnp.maximum, tops)


def iotas():
    return tuple(lax.broadcasted_iota(jnp.int32, (8, LANES), dim) for dim in range(2))


def fill_bias(bias_ref, limit):
    sub, lane = iotas()
    key = 32 * (lane >> 1) + (lane & 1) - (sub >> 2)
    for d in range(BIASES):
        bias_ref[d] = jnp.where(key > limit + 2 * (d - TILES + 1), -1e30, 0.0)


def weigh(s_ref, w_ref, m_ref, t_ref):
    for v in range(s_ref.shape[0] // 8):
        at = slice(8 * v, 8 * v + 8)
        top = m_ref[at, :]
        ws = []
        for n in range(TILES):
            w = jnp.exp2((s_ref[at, n * LANES : n * LANES + LANES] - top) * SCALE)
            w_ref[at, n * LANES : n * LANES + LANES] = w
            ws.append(w)
        t_ref[at, :] = tree(jnp.add, ws)


def row_stats(m_ref, t_ref, mt_ref):
    mt = m_ref[...].T
    mt_ref[...] = mt
    top = jnp.max(mt, axis=0, keepdims=True)
    total = jnp.sum(t_ref[...].T * jnp.exp2((mt - top) * SCALE), axis=0, keepdims=True)
    return top * SCALE + jnp.log2(total)


def accumulate(w_ref, f_ref, acc_ref):
    groups = w_ref.shape[0] // 8
    vert = [None] * TILES
    diag = [None] * TAUS
    add = lambda a, b: b if a is None else a + b
    for v in range(groups):
        at = slice(8 * v, 8 * v + 8)
        factor = f_ref[at, :]
        start = groups - 1 - v
        for n in range(TILES):
            p = w_ref[at, n * LANES : n * LANES + LANES] * factor
            vert[n] = add(vert[n], p)
            diag[start + n] = add(diag[start + n], p)
        acc_ref[start + TILES - 1] = diag[start + TILES - 1]
    for t in range(TILES - 1):
        acc_ref[t] = diag[t]
    for n in range(TILES):
        acc_ref[TAUS + n] = vert[n]


def natural(tiles):
    _, lane = iotas()
    turned = [tiles[0]] + [pltpu.roll(tiles[n], 8 * n, 1) for n in range(1, TILES)]
    turned = [turned[-n] for n in range(TILES)]
    for bit in range(4):
        step = ((lane >> (3 + bit)) & 1) == 1
        turned = [jnp.where(step, turned[n - (1 << bit)], turned[n]) for n in range(TILES)]
    return [interleaved(x, 8 * n) for n, x in enumerate(turned)]


def interleaved(x, start=0):
    _, lane = iotas()
    source = (start + ((lane >> 1) & 15) * 8 + (lane >> 5) * 2 + (lane & 1)) & (LANES - 1)
    return jnp.take_along_axis(x, source, axis=1)


def both(first, second):
    sub, _ = iotas()
    return jnp.where(sub < 4, first, second)


def folded(x):
    return x + pltpu.roll(x, 4, 0)


def whole_lanes(acc_ref):
    _, lane = iotas()
    inside, outside = [], []
    for n in range(TILES):
        x, y = acc_ref[n], None
        for c in range(1, 3):
            if TILES * c + n < TAUS:
                turned = pltpu.roll(acc_ref[TILES * c + n], 2 * c, 1)
                x = x + jnp.where(lane >= 2 * c, turned, 0.0)
                past = jnp.where(lane < 2 * c, turned, 0.0)
                y = past if y is None else y + past
        inside.append(x)
        outside.append(y)
    return inside, outside


def settle(acc_refs):
    _, lane = iotas()
    odd = (lane & 1) == 1
    turn = lambda x: pltpu.roll(x, 4, 0)
    (in0, out0), (in1, out1) = (whole_lanes(acc_ref) for acc_ref in acc_refs)
    upper = lambda xs, ys: [both(x, turn(y)) for x, y in zip(xs, ys)]
    lower = lambda xs, ys: [both(turn(x), y) for x, y in zip(xs, ys)]
    late, same = upper(in0, in1), lower(in0, in1)
    last = pltpu.roll(late[-1], 1, 1)
    overs = []
    for past in (upper(out0, out1), lower(out0, out1)):
        past = [past[0]] + [pltpu.roll(past[n], 8 * n, 1) for n in range(1, TILES)]
        overs.append(interleaved(tree(jnp.add, past)))
    over = jnp.where(lane < 1, last, pltpu.roll(overs[0], 1, 1)) + overs[1]

    def ordered():
        up = [pltpu.roll(x, 1, 1) for x in late[:-1]]
        down = [pltpu.roll(x, LANES - 1, 1) for x in late[:-1]]
        up.append(last)
        moved = [jnp.where(odd, up[0], jnp.where(lane < 1, 0.0, last))]
        moved += [jnp.where(odd, up[n], down[n - 1]) for n in range(1, TILES)]
        slash = natural([x + y for x, y in zip(moved, same)])
        vert = natural([both(*(folded(acc_ref[TAUS + n]) for acc_ref in acc_refs)) for n in range(TILES)])
        return vert, slash

    return over, ordered


def kernel(
    q_hbm, k_hbm, vo, so,
    qv, qg, kv, sa, sb, wv, mv, tv, mt, fv, acc, bias, over, over_in, st1, st2, total,
    q_sem, k_sem,
    z_send, z_recv, y_send, y_recv, c_send, c_recv,
    s1_send, s1_recv, s2_send, s2_recv, d_send, d_recv,
):
    layers = kv.shape[0]
    chunks = layers // CHUNK
    seq = lax.axis_index("seq")
    z, r = seq // NR, lax.rem(seq, NR)
    y, c = r // NC, lax.rem(r, NC)
    z_peer = lambda n: lax.rem(z + n, NZ) * NR + r
    r_peer = lambda n: z * NR + lax.rem(r + n, NR)
    ahead, behind = lax.rem(seq + 1, NZ * NR), lax.rem(seq + NZ * NR - 1, NZ * NR)
    count = lax.axis_size("seq")
    limit = so.shape[2] - LAST + jnp.where(seq == count - 1, 0, 1 << 20)

    own = pltpu.make_async_copy(q_hbm, qv, q_sem)
    own.start()

    def key_copies(layer, carry):
        rows = k_hbm.at[layer].reshape(8, 8, 4, 8, k_hbm.shape[2])
        for low in range(4):
            for m in range(8):
                pltpu.make_async_copy(
                    rows.at[:, m, :, pl.ds(2 * low, 2), :],
                    kv.at[layer, low, :, :, pl.ds(2 * m, 2), :],
                    k_sem.at[layer],
                ).start()
        return carry

    def keys_here(layer):
        pltpu.make_async_copy(kv.at[layer], kv.at[layer], k_sem.at[layer]).wait()

    barrier = pltpu.get_barrier_semaphore()
    greeted = [z_peer(n) for n in range(1, NZ)] + [r_peer(n) for n in range(1, NR)] + [ahead, behind]
    for peer in greeted:
        pl.semaphore_signal(barrier, inc=1, device_id={"seq": peer}, device_id_type=pl.DeviceIdType.MESH)

    def remote(src, dst, send, recv, peer):
        return pltpu.make_async_remote_copy(
            src_ref=src, dst_ref=dst, send_sem=send, recv_sem=recv,
            device_id={"seq": peer}, device_id_type=pl.DeviceIdType.MESH,
        )

    part = lambda k: pl.ds(CHUNK * k, CHUNK)

    def z_copy(k, n, zz):
        block = qg.at[zz, y, c, k]
        return remote(block, block, z_send.at[k, n - 1], z_recv.at[k, n - 1], z_peer(n))

    def y_copy(k, n, yy):
        block = qg.at[:, yy, c, k]
        peer = z * NR + lax.rem(y + n, NY) * NC + c
        return remote(block, block, y_send.at[k, n - 1], y_recv.at[k, n - 1], peer)

    def c_copy(k, cc):
        block = qg.at[:, :, cc, k]
        return remote(block, block, c_send.at[k], c_recv.at[k], z * NR + y * NC + 1 - c)

    def s1_copy(k, n, zz):
        block = st1.at[k, zz]
        return remote(block, block, s1_send.at[k, n - 1], s1_recv.at[k, n - 1], z_peer(n))

    def s2_copy(k, n, rr):
        block = st2.at[k, rr]
        return remote(block, block, s2_send.at[k, n - 1], s2_recv.at[k, n - 1], r_peer(n))

    def d_copy(k):
        return remote(over.at[part(k)], over_in.at[part(k)], d_send.at[k], d_recv.at[k], ahead)

    def z_to_y(k):
        for n in range(1, NZ):
            z_copy(k, n, lax.rem(z + NZ - n, NZ)).wait_recv()
        for n in range(1, NY):
            y_copy(k, n, y).start()

    def y_to_c(k):
        for n in range(1, NY):
            y_copy(k, n, lax.rem(y + NY - n, NY)).wait_recv()
        c_copy(k, c).start()

    def s1_to_s2(k):
        for n in range(1, NZ):
            s1_copy(k, n, lax.rem(z + NZ - n, NZ)).wait_recv()
        st2[k, r] = combined([st1[k, n] for n in range(NZ)])
        for n in range(1, NR):
            s2_copy(k, n, r).start()

    def queries(layer, group):
        return qg[:, :, :, layer, group].reshape(-1, HD)

    lax.fori_loop(0, CHUNK, key_copies, 0)
    own.wait()
    block = qv[...].astype(F32).reshape(layers, -1, HD).astype(BF16)
    qg[z, y, c] = block.reshape(qg.shape[3:])
    fill_bias(bias, limit)
    pl.semaphore_wait(barrier, len(greeted))
    def z_starts(k, carry):
        for n in range(1, NZ):
            z_copy(k, n, z).start()
        return carry

    lax.fori_loop(0, layers, z_starts, 0)
    lax.fori_loop(CHUNK, layers, key_copies, 0)

    def z_passes(k, carry):
        z_to_y(k)
        return carry

    lax.fori_loop(0, layers, z_passes, 0)
    y_to_c(0)
    y_to_c(1)
    keys_here(0)
    c_copy(0, 1 - c).wait_recv()
    score(queries(0, 0), kv, 0, 0, sa, mv.at[0], bias)

    def gather_stats(k, row, m_ref, t_ref, mt_ref):
        found = row_stats(m_ref, t_ref, mt_ref)
        for half in range(2):
            st1[k, z, pl.ds(2 * row + half, 1), :] = found[:, half * LANES : half * LANES + LANES]

    def first_pass(k, carry):
        def layer_pass(j, carry):
            layer = CHUNK * k + j
            following = jnp.minimum(layer + 1, layers - 1)
            score(queries(layer, 1), kv, layer, 1, sb, mv.at[1], bias)
            weigh(sa, wv.at[layer, 0], mv.at[0], tv.at[0])
            gather_stats(k, 2 * j, mv.at[0], tv.at[0], mt.at[layer, 0])

            @pl.when(layer + 2 < layers)
            def _():
                y_to_c(layer + 2)

            @pl.when(layer + 1 < layers)
            def _():
                keys_here(layer + 1)
                c_copy(layer + 1, 1 - c).wait_recv()

            score(queries(following, 0), kv, following, 0, sa, mv.at[0], bias)
            weigh(sb, wv.at[layer, 1], mv.at[1], tv.at[1])
            gather_stats(k, 2 * j + 1, mv.at[1], tv.at[1], mt.at[layer, 1])
            return carry

        lax.fori_loop(0, CHUNK, layer_pass, 0)
        for n in range(1, NZ):
            s1_copy(k, n, z).start()

        @pl.when(k > 1)
        def _():
            s1_to_s2(k - 2)

        return carry

    lax.fori_loop(0, chunks, first_pass, 0)

    def finish(k):
        d_copy(k).wait_recv()
        for j in range(CHUNK):
            so[CHUNK * k + j, :, 0:LANES] = so[CHUNK * k + j, :, 0:LANES] + over_in[CHUNK * k + j]

    def second_pass(k, carry):
        for n in range(1, NR):
            s2_copy(k, n, lax.rem(r + NR - n, NR)).wait_recv()
        total[...] = math.log2(so.shape[2] * count / LAST) - combined([st2[k, n] for n in range(NR)])
        for j in range(CHUNK):
            for group in range(2):
                for half in range(2):
                    at = slice(half * LANES, half * LANES + LANES)
                    row = 4 * j + 2 * group + half
                    logs = mt[CHUNK * k + j, group, :, at] * SCALE + total[row : row + 1, :]
                    fv[j, group, at, :] = jnp.exp2(logs).T

        def sums(n, carry):
            j, group = n // 2, lax.rem(n, 2)
            accumulate(wv.at[CHUNK * k + j, group], fv.at[j, group], acc.at[j, group])
            return carry

        lax.fori_loop(0, 2 * CHUNK, sums, 0)
        rest = []
        for j in range(CHUNK):
            over[CHUNK * k + j], ordered = settle([acc.at[j, 0], acc.at[j, 1]])
            rest.append(ordered)
        d_copy(k).start()
        for j in range(CHUNK):
            for ref, tiles in zip((vo, so), rest[j]()):
                for n in range(TILES):
                    ref[CHUNK * k + j, :, n * LANES : n * LANES + LANES] = tiles[n]

        @pl.when(k < 2)
        def _():
            s1_to_s2(chunks - 2 + k)

        @pl.when(k > 1)
        def _():
            finish(k - 2)

        return carry

    lax.fori_loop(0, chunks, second_pass, 0)
    finish(chunks - 2)
    finish(chunks - 1)

    def drain(k, carry):
        for n in range(1, NZ):
            z_copy(k, n, z).wait_send()
        for n in range(1, NY):
            y_copy(k, n, y).wait_send()
        c_copy(k, c).wait_send()
        return carry

    def drain_stats(k, carry):
        for n in range(1, NZ):
            s1_copy(k, n, z).wait_send()
        for n in range(1, NR):
            s2_copy(k, n, r).wait_send()
        d_copy(k).wait_send()
        return carry

    lax.fori_loop(0, layers, drain, 0)
    lax.fori_loop(0, chunks, drain_stats, 0)


def on_device(tail_queries, keys):
    layers, key_count, width = keys.shape
    groups = width // HD
    heads = tail_queries.shape[2] // HD
    per_group = heads // groups
    rows = LAST * per_group
    chunks = layers // CHUNK
    q = tail_queries.reshape(layers, heads * HD)
    out = pltpu.VMEM((layers, heads, key_count), F32)
    dma = pltpu.SemaphoreType.DMA
    return pl.pallas_call(
        kernel,
        out_shape=(out, out),
        in_specs=[pl.BlockSpec(memory_space=pl.ANY)] * 2,
        out_specs=[pl.BlockSpec(memory_space=pltpu.VMEM)] * 2,
        scratch_shapes=[
            pltpu.VMEM((layers, heads * HD), BF16),
            pltpu.VMEM((NZ, NY, NC, layers, groups, per_group, HD), BF16),
            pltpu.VMEM((layers, 4, 8, 4, 16, width), BF16),
            pltpu.VMEM((rows, key_count), F32),
            pltpu.VMEM((rows, key_count), F32),
            pltpu.VMEM((layers, groups, rows, key_count), F32),
            pltpu.VMEM((groups, rows, LANES), F32),
            pltpu.VMEM((groups, rows, LANES), F32),
            pltpu.VMEM((layers, groups, LANES, rows), F32),
            pltpu.VMEM((CHUNK, groups, rows, LANES), F32),
            pltpu.VMEM((CHUNK, groups, TAUS + TILES, 8, LANES), F32),
            pltpu.VMEM((BIASES, 8, LANES), F32),
            pltpu.VMEM((layers, heads, LANES), F32),
            pltpu.VMEM((layers, heads, LANES), F32),
            pltpu.VMEM((chunks, NZ, 8, LANES), F32),
            pltpu.VMEM((chunks, NR, 8, LANES), F32),
            pltpu.VMEM((8, LANES), F32),
            dma,
            dma((layers,)),
            dma((layers, NZ - 1)),
            dma((layers, NZ - 1)),
            dma((layers, NY - 1)),
            dma((layers, NY - 1)),
            dma((layers,)),
            dma((layers,)),
            dma((chunks, NZ - 1)),
            dma((chunks, NZ - 1)),
            dma((chunks, NR - 1)),
            dma((chunks, NR - 1)),
            dma((chunks,)),
            dma((chunks,)),
        ],
        compiler_params=pltpu.CompilerParams(
            collective_id=0, has_side_effects=True, vmem_limit_bytes=64600000
        ),
    )(q, keys)


def solution(mesh):
    return jax.shard_map(
        on_device,
        mesh=mesh,
        in_specs=(P(None, "seq", "head"), P(None, "seq", "head")),
        out_specs=(P(None, "head", "seq"), P(None, "head", "seq")),
        check_vma=False,
    )
```

```python
import functools
import math

import jax
import jax.numpy as jnp
from jax import lax
from jax.experimental import pallas as pl
from jax.experimental.pallas import tpu as pltpu
from jax.sharding import PartitionSpec as P

HD = 128
LAST = 64
LANES = 128
F32 = jnp.float32
BF16 = jnp.bfloat16
SCALE = math.log2(math.e) / math.sqrt(HD)
CHUNK = 2
NZ, NY, NC = 8, 4, 2
NR = NY * NC
TILES = 16
TAUS = TILES + LAST // 2 - 1
BIASES = 2 * TILES


def tree(op, xs):
    xs = list(xs)
    while len(xs) > 1:
        xs = [op(*xs[n : n + 2]) if n + 1 < len(xs) else xs[n] for n in range(0, len(xs), 2)]
    return xs[0]


def combined(parts):
    top = tree(jnp.maximum, parts)
    return top + jnp.log2(tree(jnp.add, [jnp.exp2(part - top) for part in parts]))


def score(q, k_ref, layer, group, s_ref, m_ref, bias_ref):
    tile = lambda n: k_ref[layer, n % 4, :, n // 4, :, HD * group : HD * group + HD].reshape(LANES, HD)
    for n in range(0, TILES, 4):
        k = jnp.concatenate([tile(n + i) for i in range(4)], axis=0)
        x = lax.dot_general(q, k, (((1,), (1,)), ((), ())), preferred_element_type=F32)
        for v in range(q.shape[0] // 8):
            at = slice(8 * v, 8 * v + 8)
            tops = [m_ref[at, :]] if n else []
            for i in range(4):
                y = x[at, i * LANES : i * LANES + LANES]
                d = v - n - i + TILES - 1
                if d < BIASES:
                    y = y + bias_ref[d]
                s_ref[at, (n + i) * LANES : (n + i + 1) * LANES] = y
                tops.append(y)
            m_ref[at, :] = tree(jnp.maximum, tops)


def iotas():
    return tuple(lax.broadcasted_iota(jnp.int32, (8, LANES), dim) for dim in range(2))


def fill_bias(bias_ref, limit):
    sub, lane = iotas()
    key = 32 * (lane >> 1) + (lane & 1) - (sub >> 2)
    for d in range(BIASES):
        bias_ref[d] = jnp.where(key > limit + 2 * (d - TILES + 1), -1e30, 0.0)


def weigh(s_ref, w_ref, m_ref, t_ref):
    for v in range(s_ref.shape[0] // 8):
        at = slice(8 * v, 8 * v + 8)
        top = m_ref[at, :]
        ws = []
        for n in range(TILES):
            w = jnp.exp2((s_ref[at, n * LANES : n * LANES + LANES] - top) * SCALE)
            w_ref[at, n * LANES : n * LANES + LANES] = w
            ws.append(w)
        t_ref[at, :] = tree(jnp.add, ws)


def row_stats(m_ref, t_ref, mt_ref):
    mt = m_ref[...].T
    mt_ref[...] = mt
    top = jnp.max(mt, axis=0, keepdims=True)
    total = jnp.sum(t_ref[...].T * jnp.exp2((mt - top) * SCALE), axis=0, keepdims=True)
    return top * SCALE + jnp.log2(total)


def accumulate(w_ref, f_ref, acc_ref):
    groups = w_ref.shape[0] // 8
    vert = [None] * TILES
    diag = [None] * TAUS
    add = lambda a, b: b if a is None else a + b
    for v in range(groups):
        at = slice(8 * v, 8 * v + 8)
        factor = f_ref[at, :]
        start = groups - 1 - v
        for n in range(TILES):
            p = w_ref[at, n * LANES : n * LANES + LANES] * factor
            vert[n] = add(vert[n], p)
            diag[start + n] = add(diag[start + n], p)
        acc_ref[start + TILES - 1] = diag[start + TILES - 1]
    for t in range(TILES - 1):
        acc_ref[t] = diag[t]
    for n in range(TILES):
        acc_ref[TAUS + n] = vert[n]


def natural(tiles):
    _, lane = iotas()
    turned = [tiles[0]] + [pltpu.roll(tiles[n], 8 * n, 1) for n in range(1, TILES)]
    turned = [turned[-n] for n in range(TILES)]
    for bit in range(4):
        step = ((lane >> (3 + bit)) & 1) == 1
        turned = [jnp.where(step, turned[n - (1 << bit)], turned[n]) for n in range(TILES)]
    return [interleaved(x, 8 * n) for n, x in enumerate(turned)]


def interleaved(x, start=0):
    _, lane = iotas()
    source = (start + ((lane >> 1) & 15) * 8 + (lane >> 5) * 2 + (lane & 1)) & (LANES - 1)
    return jnp.take_along_axis(x, source, axis=1)


def both(first, second):
    sub, _ = iotas()
    return jnp.where(sub < 4, first, second)


def folded(x):
    return x + pltpu.roll(x, 4, 0)


def whole_lanes(acc_ref):
    _, lane = iotas()
    inside, outside = [], []
    for n in range(TILES):
        x, y = acc_ref[n], None
        for c in range(1, 3):
            if TILES * c + n < TAUS:
                turned = pltpu.roll(acc_ref[TILES * c + n], 2 * c, 1)
                x = x + jnp.where(lane >= 2 * c, turned, 0.0)
                past = jnp.where(lane < 2 * c, turned, 0.0)
                y = past if y is None else y + past
        inside.append(x)
        outside.append(y)
    return inside, outside


def settle(acc_refs):
    _, lane = iotas()
    odd = (lane & 1) == 1
    turn = lambda x: pltpu.roll(x, 4, 0)
    (in0, out0), (in1, out1) = (whole_lanes(acc_ref) for acc_ref in acc_refs)
    upper = lambda xs, ys: [both(x, turn(y)) for x, y in zip(xs, ys)]
    lower = lambda xs, ys: [both(turn(x), y) for x, y in zip(xs, ys)]
    late, same = upper(in0, in1), lower(in0, in1)
    last = pltpu.roll(late[-1], 1, 1)
    overs = []
    for past in (upper(out0, out1), lower(out0, out1)):
        past = [past[0]] + [pltpu.roll(past[n], 8 * n, 1) for n in range(1, TILES)]
        overs.append(interleaved(tree(jnp.add, past)))
    over = jnp.where(lane < 1, last, pltpu.roll(overs[0], 1, 1)) + overs[1]

    def ordered():
        up = [pltpu.roll(x, 1, 1) for x in late[:-1]]
        down = [pltpu.roll(x, LANES - 1, 1) for x in late[:-1]]
        up.append(last)
        moved = [jnp.where(odd, up[0], jnp.where(lane < 1, 0.0, last))]
        moved += [jnp.where(odd, up[n], down[n - 1]) for n in range(1, TILES)]
        slash = natural([x + y for x, y in zip(moved, same)])
        vert = natural([both(*(folded(acc_ref[TAUS + n]) for acc_ref in acc_refs)) for n in range(TILES)])
        return vert, slash

    return over, ordered


def kernel(
    q_hbm, k_hbm, vo, so,
    qv, qg, kv, sa, sb, wv, mv, tv, mt, fv, acc, bias, over, over_in, st1, st2, total,
    q_sem, k_sem,
    z_send, z_recv, y_send, y_recv, c_send, c_recv,
    s1_send, s1_recv, s2_send, s2_recv, d_send, d_recv,
):
    layers = kv.shape[0]
    chunks = layers // CHUNK
    seq = lax.axis_index("seq")
    z, r = seq // NR, lax.rem(seq, NR)
    y, c = r // NC, lax.rem(r, NC)
    z_peer = lambda n: lax.rem(z + n, NZ) * NR + r
    r_peer = lambda n: z * NR + lax.rem(r + n, NR)
    ahead, behind = lax.rem(seq + 1, NZ * NR), lax.rem(seq + NZ * NR - 1, NZ * NR)
    count = lax.axis_size("seq")
    limit = so.shape[2] - LAST + jnp.where(seq == count - 1, 0, 1 << 20)

    own = pltpu.make_async_copy(q_hbm, qv, q_sem)
    own.start()

    def key_copies(layer, carry):
        rows = k_hbm.at[layer].reshape(8, 8, 4, 8, k_hbm.shape[2])
        for low in range(4):
            for m in range(8):
                pltpu.make_async_copy(
                    rows.at[:, m, :, pl.ds(2 * low, 2), :],
                    kv.at[layer, low, :, :, pl.ds(2 * m, 2), :],
                    k_sem.at[layer],
                ).start()
        return carry

    def keys_here(layer):
        pltpu.make_async_copy(kv.at[layer], kv.at[layer], k_sem.at[layer]).wait()

    barrier = pltpu.get_barrier_semaphore()
    greeted = [z_peer(n) for n in range(1, NZ)] + [r_peer(n) for n in range(1, NR)] + [ahead, behind]
    for peer in greeted:
        pl.semaphore_signal(barrier, inc=1, device_id={"seq": peer}, device_id_type=pl.DeviceIdType.MESH)

    def remote(src, dst, send, recv, peer):
        return pltpu.make_async_remote_copy(
            src_ref=src, dst_ref=dst, send_sem=send, recv_sem=recv,
            device_id={"seq": peer}, device_id_type=pl.DeviceIdType.MESH,
        )

    part = lambda k: pl.ds(CHUNK * k, CHUNK)

    def z_copy(k, n, zz):
        block = qg.at[zz, y, c, k]
        return remote(block, block, z_send.at[k, n - 1], z_recv.at[k, n - 1], z_peer(n))

    def y_copy(k, n, yy):
        block = qg.at[:, yy, c, k]
        peer = z * NR + lax.rem(y + n, NY) * NC + c
        return remote(block, block, y_send.at[k, n - 1], y_recv.at[k, n - 1], peer)

    def c_copy(k, cc):
        block = qg.at[:, :, cc, k]
        return remote(block, block, c_send.at[k], c_recv.at[k], z * NR + y * NC + 1 - c)

    def s1_copy(k, n, zz):
        block = st1.at[k, zz]
        return remote(block, block, s1_send.at[k, n - 1], s1_recv.at[k, n - 1], z_peer(n))

    def s2_copy(k, n, rr):
        block = st2.at[k, rr]
        return remote(block, block, s2_send.at[k, n - 1], s2_recv.at[k, n - 1], r_peer(n))

    def d_copy(k):
        return remote(over.at[part(k)], over_in.at[part(k)], d_send.at[k], d_recv.at[k], ahead)

    def z_to_y(k):
        for n in range(1, NZ):
            z_copy(k, n, lax.rem(z + NZ - n, NZ)).wait_recv()
        for n in range(1, NY):
            y_copy(k, n, y).start()

    def y_to_c(k):
        for n in range(1, NY):
            y_copy(k, n, lax.rem(y + NY - n, NY)).wait_recv()
        c_copy(k, c).start()

    def s1_to_s2(k):
        for n in range(1, NZ):
            s1_copy(k, n, lax.rem(z + NZ - n, NZ)).wait_recv()
        st2[k, r] = combined([st1[k, n] for n in range(NZ)])
        for n in range(1, NR):
            s2_copy(k, n, r).start()

    def queries(layer, group):
        return qg[:, :, :, layer, group].reshape(-1, HD)

    lax.fori_loop(0, CHUNK, key_copies, 0)
    own.wait()
    block = qv[...].astype(F32).reshape(layers, -1, HD).astype(BF16)
    qg[z, y, c] = block.reshape(qg.shape[3:])
    fill_bias(bias, limit)
    pl.semaphore_wait(barrier, len(greeted))
    def z_starts(k, carry):
        for n in range(1, NZ):
            z_copy(k, n, z).start()
        return carry

    lax.fori_loop(0, layers, z_starts, 0)
    lax.fori_loop(CHUNK, layers, key_copies, 0)

    def z_passes(k, carry):
        z_to_y(k)
        return carry

    lax.fori_loop(0, layers, z_passes, 0)
    y_to_c(0)
    y_to_c(1)
    keys_here(0)
    c_copy(0, 1 - c).wait_recv()
    score(queries(0, 0), kv, 0, 0, sa, mv.at[0], bias)

    def gather_stats(k, row, m_ref, t_ref, mt_ref):
        found = row_stats(m_ref, t_ref, mt_ref)
        for half in range(2):
            st1[k, z, pl.ds(2 * row + half, 1), :] = found[:, half * LANES : half * LANES + LANES]

    def first_pass(k, carry):
        def layer_pass(j, carry):
            layer = CHUNK * k + j
            following = jnp.minimum(layer + 1, layers - 1)
            score(queries(layer, 1), kv, layer, 1, sb, mv.at[1], bias)
            weigh(sa, wv.at[layer, 0], mv.at[0], tv.at[0])
            gather_stats(k, 2 * j, mv.at[0], tv.at[0], mt.at[layer, 0])

            @pl.when(layer + 2 < layers)
            def _():
                y_to_c(layer + 2)

            @pl.when(layer + 1 < layers)
            def _():
                keys_here(layer + 1)
                c_copy(layer + 1, 1 - c).wait_recv()

            score(queries(following, 0), kv, following, 0, sa, mv.at[0], bias)
            weigh(sb, wv.at[layer, 1], mv.at[1], tv.at[1])
            gather_stats(k, 2 * j + 1, mv.at[1], tv.at[1], mt.at[layer, 1])
            return carry

        lax.fori_loop(0, CHUNK, layer_pass, 0)
        for n in range(1, NZ):
            s1_copy(k, n, z).start()

        @pl.when(k > 1)
        def _():
            s1_to_s2(k - 2)

        return carry

    lax.fori_loop(0, chunks, first_pass, 0)

    def finish(k):
        d_copy(k).wait_recv()
        for j in range(CHUNK):
            so[CHUNK * k + j, :, 0:LANES] = so[CHUNK * k + j, :, 0:LANES] + over_in[CHUNK * k + j]

    def second_pass(k, carry):
        for n in range(1, NR):
            s2_copy(k, n, lax.rem(r + NR - n, NR)).wait_recv()
        total[...] = math.log2(so.shape[2] * count / LAST) - combined([st2[k, n] for n in range(NR)])
        for j in range(CHUNK):
            for group in range(2):
                for half in range(2):
                    at = slice(half * LANES, half * LANES + LANES)
                    row = 4 * j + 2 * group + half
                    logs = mt[CHUNK * k + j, group, :, at] * SCALE + total[row : row + 1, :]
                    fv[j, group, at, :] = jnp.exp2(logs).T

        def sums(n, carry):
            j, group = n // 2, lax.rem(n, 2)
            accumulate(wv.at[CHUNK * k + j, group], fv.at[j, group], acc.at[j, group])
            return carry

        lax.fori_loop(0, 2 * CHUNK, sums, 0)
        rest = []
        for j in range(CHUNK):
            over[CHUNK * k + j], ordered = settle([acc.at[j, 0], acc.at[j, 1]])
            rest.append(ordered)
        d_copy(k).start()
        for j in range(CHUNK):
            for ref, tiles in zip((vo, so), rest[j]()):
                for n in range(TILES):
                    ref[CHUNK * k + j, :, n * LANES : n * LANES + LANES] = tiles[n]

        @pl.when(k < 2)
        def _():
            s1_to_s2(chunks - 2 + k)

        @pl.when(k > 1)
        def _():
            finish(k - 2)

        return carry

    lax.fori_loop(0, chunks, second_pass, 0)
    finish(chunks - 2)
    finish(chunks - 1)

    def drain(k, carry):
        for n in range(1, NZ):
            z_copy(k, n, z).wait_send()
        for n in range(1, NY):
            y_copy(k, n, y).wait_send()
        c_copy(k, c).wait_send()
        return carry

    def drain_stats(k, carry):
        for n in range(1, NZ):
            s1_copy(k, n, z).wait_send()
        for n in range(1, NR):
            s2_copy(k, n, r).wait_send()
        d_copy(k).wait_send()
        return carry

    lax.fori_loop(0, layers, drain, 0)
    lax.fori_loop(0, chunks, drain_stats, 0)


def write_out(vert_ref, slash_ref, vert_hbm, slash_hbm, sem):
    copies = [
        pltpu.make_async_copy(vert_ref, vert_hbm, sem.at[0]),
        pltpu.make_async_copy(slash_ref, slash_hbm, sem.at[1]),
    ]
    for copy in copies:
        copy.start()
    for copy in copies:
        copy.wait()


def on_device(tail_queries, keys):
    layers, key_count, width = keys.shape
    groups = width // HD
    heads = tail_queries.shape[2] // HD
    per_group = heads // groups
    rows = LAST * per_group
    chunks = layers // CHUNK
    q = tail_queries.reshape(layers, heads * HD)
    out = pltpu.VMEM((layers, heads, key_count), F32)
    dma = pltpu.SemaphoreType.DMA
    sums = pl.pallas_call(
        kernel,
        out_shape=(out, out),
        in_specs=[pl.BlockSpec(memory_space=pl.ANY)] * 2,
        out_specs=[pl.BlockSpec(memory_space=pltpu.VMEM)] * 2,
        scratch_shapes=[
            pltpu.VMEM((layers, heads * HD), BF16),
            pltpu.VMEM((NZ, NY, NC, layers, groups, per_group, HD), BF16),
            pltpu.VMEM((layers, 4, 8, 4, 16, width), BF16),
            pltpu.VMEM((rows, key_count), F32),
            pltpu.VMEM((rows, key_count), F32),
            pltpu.VMEM((layers, groups, rows, key_count), F32),
            pltpu.VMEM((groups, rows, LANES), F32),
            pltpu.VMEM((groups, rows, LANES), F32),
            pltpu.VMEM((layers, groups, LANES, rows), F32),
            pltpu.VMEM((CHUNK, groups, rows, LANES), F32),
            pltpu.VMEM((CHUNK, groups, TAUS + TILES, 8, LANES), F32),
            pltpu.VMEM((BIASES, 8, LANES), F32),
            pltpu.VMEM((layers, heads, LANES), F32),
            pltpu.VMEM((layers, heads, LANES), F32),
            pltpu.VMEM((chunks, NZ, 8, LANES), F32),
            pltpu.VMEM((chunks, NR, 8, LANES), F32),
            pltpu.VMEM((8, LANES), F32),
            dma,
            dma((layers,)),
            dma((layers, NZ - 1)),
            dma((layers, NZ - 1)),
            dma((layers, NY - 1)),
            dma((layers, NY - 1)),
            dma((layers,)),
            dma((layers,)),
            dma((chunks, NZ - 1)),
            dma((chunks, NZ - 1)),
            dma((chunks, NR - 1)),
            dma((chunks, NR - 1)),
            dma((chunks,)),
            dma((chunks,)),
        ],
        compiler_params=pltpu.CompilerParams(
            collective_id=0, has_side_effects=True, vmem_limit_bytes=64600000
        ),
    )(q, keys)
    return pl.pallas_call(
        write_out,
        out_shape=(jax.ShapeDtypeStruct((layers, heads, key_count), F32),) * 2,
        in_specs=[pl.BlockSpec(memory_space=pl.ANY)] * 2,
        out_specs=[pl.BlockSpec(memory_space=pl.ANY)] * 2,
        scratch_shapes=[dma((2,))],
        compiler_params=pltpu.CompilerParams(vmem_limit_bytes=1 << 20),
    )(*sums)


def solution(mesh):
    return jax.shard_map(
        on_device,
        mesh=mesh,
        in_specs=(P(None, "seq", "head"), P(None, "seq", "head")),
        out_specs=(P(None, "head", "seq"), P(None, "head", "seq")),
        check_vma=False,
    )
```
